32 devices in a mesh: col: 4 (over z), row: 8 (over y, x, core).
Axes of the slice: x: 2, y: 2, z: 4, core: 2. Of those that a mesh axis runs over, the one named last changes fastest.
Arguments:
- queries: bfloat16 [32768, 256], P(('col', 'row')), may hold values from -6 to 6
- keys: bfloat16 [32768, 256], P(('col', 'row')), may hold values from -6 to 6
- values: bfloat16 [32768, 256], P(('col', 'row')), may hold values from -6 to 6
- out_grad: bfloat16 [32768, 256], P(('col', 'row')), may hold values from -6 to 6
- weight_table: float32 [64, 2, 21], replicated, may hold values from 0.25 to 2
- profile: int32 [32768], P(('col', 'row')), may hold values from 0 to 63
Outputs:
- output: float32 [32768, 256], P(('col', 'row'))
- query_grad: float32 [32768, 256], P(('col', 'row'))
- key_grad: float32 [32768, 256], P(('col', 'row'))
- value_grad: float32 [32768, 256], P(('col', 'row'))
The draws below stay inside these ranges and needn't reach their ends.
All inputs are finite; a program needn't handle non-finite values.
Results may differ from the reference program's by a relative error of at most 0.0034.
Values sent between devices are 32-bit elements; how exact they have to be, the bound alone decides.
A program may use at most 128 MiB of HBM per device.

```python
import math
import jax
import jax.numpy as jnp
from jax import lax

H = 2
DH = 128
LEVELS = 21
PROFILES = 64
SEQ = 32768
N_COL = 4
N_ROW = 8


def with_ends(array, own_key, smallest, high):
    shape = array.shape
    spot = [jax.random.randint(jax.random.fold_in(own_key, axis), (), 0, shape[axis]) for axis in range(len(shape))]
    array = array.at[tuple(spot)].set(smallest)
    longest = shape.index(max(shape))
    spot[longest] = (spot[longest] + 1) % shape[longest]
    return array.at[tuple(spot)].set(high)


def shard_levels(key, extent, split, low, largest):
    def one(position, shards_of):
        steps = jax.random.uniform(jax.random.fold_in(jax.random.fold_in(key, 6), position), (shards_of,), jnp.float32, low / len(split), largest / len(split))
        return jnp.repeat(jnp.exp(steps), extent[position] // shards_of).reshape((-1,) + (1,) * (len(extent) - position - 1))

    gain = one(*split[0])
    for cut in split[1:]:
        gain = gain * one(*cut)
    return gain


def scatter_about(rng, dims, scale, most, shards=(), kind=jnp.bfloat16):
    array = scale * jax.random.normal(rng, dims, jnp.float32)
    if shards:
        array = array * shard_levels(rng, dims, shards, -0.22, 0.18)
    return jnp.clip(array, -most, most).astype(kind)


def setup_inputs(seed: int = 0) -> dict:
    key_of = jax.random.split(jax.random.key(seed), 7)
    return {
        "queries": scatter_about(key_of[0], (SEQ, H * DH), 1.0, 6.0, ((0, 32),)),
        "keys": scatter_about(key_of[1], (SEQ, H * DH), 1.0, 6.0, ((0, 32),)),
        "values": scatter_about(key_of[2], (SEQ, H * DH), 1.0, 6.0, ((0, 32),)),
        "out_grad": scatter_about(key_of[3], (SEQ, H * DH), 1.0, 6.0, ((0, 32),)),
        "weight_table": jnp.clip(jnp.exp(jax.random.uniform(key_of[4], (PROFILES, H, LEVELS), jnp.float32, math.log(0.25), math.log(2.0))), 0.25, 2.0),
        "profile": with_ends(jax.random.randint(key_of[5], (SEQ,), 0, PROFILES), jax.random.fold_in(key_of[5], 1), 0, PROFILES - 1).astype(jnp.int32),
    }


HIGHEST_PRECISION = lax.Precision.HIGHEST

def digit_count(numbers, count):
    total = jnp.zeros_like(numbers)
    for digit_place in range(count):
        total = total + (numbers >= 1 << digit_place).astype(jnp.int32)
    return total

def level_weights(weight_table, profile, head_width):
    table_rows = weight_table.shape[0]
    onehot = (profile[:, None] == jnp.arange(table_rows, dtype=jnp.int32)[None, :]).astype(jnp.float32)
    flat_table = weight_table.reshape(table_rows, -1)
    picked = jnp.dot(onehot, flat_table, precision=HIGHEST_PRECISION, preferred_element_type=jnp.float32)
    picked = picked.reshape(profile.shape[0], weight_table.shape[1], weight_table.shape[2])
    depth = jnp.arange(weight_table.shape[2], dtype=jnp.float32)
    scaling = jnp.exp2(-0.5 * depth) / math.sqrt(head_width)
    return picked * scaling

def sibling_sums(states, bit_place, receiver):
    count = states.shape[0]
    remain = states.shape[1:]
    shape = (count >> bit_place + 1, 2, 1 << bit_place) + remain
    grouped = lax.optimization_barrier(jnp.sum(states.reshape(shape), axis=2))
    source = grouped[:, 1 - receiver]
    empty = jnp.zeros_like(source)
    halves = [source, empty] if receiver == 0 else [empty, source]
    paired = jnp.stack(halves, axis=1)
    spread = jnp.broadcast_to(paired[:, :, None], shape)
    return spread.reshape(states.shape)

def tile_local(query_heads, key_heads, value_heads, grad_heads, weights, tile_bits):
    count = query_heads.shape[0]
    places = jnp.arange(count, dtype=jnp.int32)
    levels = digit_count(jnp.bitwise_xor(places[:, None], places[None, :]), tile_bits)
    causal = places[None, :] <= places[:, None]
    level_mask = jnp.zeros((query_heads.shape[1], count, count), jnp.float32)
    for level in range(tile_bits + 1):
        level_mask = level_mask + jnp.where(levels[None] == level, jnp.transpose(weights[:, :, level])[:, :, None], 0.0)
    level_mask = jnp.where(causal[None], level_mask, 0.0)
    query_f = query_heads.astype(jnp.float32)
    key_f = key_heads.astype(jnp.float32)
    value_f = value_heads.astype(jnp.float32)
    grad_f = grad_heads.astype(jnp.float32)
    scores = jnp.einsum('thd,shd->hts', query_f, key_f, precision=HIGHEST_PRECISION)
    local_probs = (scores * level_mask).astype(jnp.bfloat16)
    probs_f = local_probs.astype(jnp.float32)
    local_out = jnp.einsum('hts,she->the', probs_f, value_f, precision=HIGHEST_PRECISION)
    grad_scores = jnp.einsum('the,she->hts', grad_f, value_f, precision=HIGHEST_PRECISION)
    local_grad = (grad_scores * level_mask).astype(jnp.bfloat16).astype(jnp.float32)
    local_dq = jnp.einsum('hts,shd->thd', local_grad, key_f, precision=HIGHEST_PRECISION)
    local_dk = jnp.einsum('hts,thd->shd', local_grad, query_f, precision=HIGHEST_PRECISION)
    local_dv = jnp.einsum('hts,the->she', probs_f, grad_f, precision=HIGHEST_PRECISION)
    return (local_out, local_dq, local_dk, local_dv)

def tile_far(query_heads, key_heads, value_heads, grad_heads, far_weights, bucket_half, pulled_half):
    query_f = query_heads.astype(jnp.float32)
    key_f = key_heads.astype(jnp.float32)
    value_f = value_heads.astype(jnp.float32)
    grad_f = grad_heads.astype(jnp.float32)
    bucket_f = bucket_half.astype(jnp.float32)
    pulled_f = pulled_half.astype(jnp.float32)
    reach = jnp.einsum('thd,lhde->thle', query_f, bucket_f, precision=HIGHEST_PRECISION)
    far_out = lax.optimization_barrier(jnp.sum(reach * far_weights[..., None], axis=2))
    back = jnp.einsum('the,lhde->thld', grad_f, bucket_f, precision=HIGHEST_PRECISION)
    far_dq = lax.optimization_barrier(jnp.sum(back * far_weights[..., None], axis=2))
    far_dk = jnp.einsum('the,hde->thd', value_f, pulled_f, precision=HIGHEST_PRECISION)
    far_dv = jnp.einsum('thd,hde->the', key_f, pulled_f, precision=HIGHEST_PRECISION)
    return (far_out, far_dq, far_dk, far_dv)

def tile_grad_state(query_heads, grad_heads, far_weights):
    weighted = (query_heads.astype(jnp.float32)[:, :, None, :] * far_weights[..., None]).astype(jnp.bfloat16)
    return jnp.einsum('thld,the->lhde', weighted.astype(jnp.float32), grad_heads.astype(jnp.float32), precision=HIGHEST_PRECISION)

def reference(queries, keys, values, out_grad, weight_table, profile):
    tile_count = N_COL * N_ROW
    token_count = queries.shape[0] // tile_count
    head_count = weight_table.shape[1]
    head_width = queries.shape[1] // head_count
    tile_bits = token_count.bit_length() - 1
    far_levels = tile_count.bit_length() - 1
    weights = level_weights(weight_table, profile, head_width).reshape(tile_count, token_count, head_count, -1)
    far_weights = weights[:, :, :, tile_bits + 1:tile_bits + 1 + far_levels]
    tile_shape = (tile_count, token_count, head_count, head_width)
    query_tiles = queries.reshape(tile_shape)
    key_tiles = keys.reshape(tile_shape)
    value_tiles = values.reshape(tile_shape)
    grad_tiles = out_grad.reshape(tile_shape)
    tile_state = jnp.einsum('bthd,bthe->bhde', key_tiles.astype(jnp.float32), value_tiles.astype(jnp.float32), precision=HIGHEST_PRECISION)

    def grad_of_tile(items):
        return tile_grad_state(items[0], items[1], items[2])
    grad_state = lax.map(grad_of_tile, (query_tiles, grad_tiles, far_weights))
    bucket = jnp.stack([sibling_sums(tile_state, level, 1) for level in range(far_levels)], axis=1)
    bucket_half = bucket.astype(jnp.bfloat16)
    pulled = jnp.zeros_like(tile_state)
    for level in range(far_levels):
        pulled = pulled + sibling_sums(grad_state[:, level], level, 0)
    pulled_half = pulled.astype(jnp.bfloat16)

    def per_tile(items):
        query_heads, key_heads, value_heads, grad_heads, tile_weights, bucket_tile, pulled_tile = items
        local_out, local_dq, local_dk, local_dv = tile_local(query_heads, key_heads, value_heads, grad_heads, tile_weights, tile_bits)
        far_out, far_dq, far_dk, far_dv = tile_far(query_heads, key_heads, value_heads, grad_heads, tile_weights[:, :, tile_bits + 1:tile_bits + 1 + far_levels], bucket_tile, pulled_tile)
        return (local_out + far_out, local_dq + far_dq, local_dk + far_dk, local_dv + far_dv)
    results = lax.map(per_tile, (query_tiles, key_tiles, value_tiles, grad_tiles, weights, bucket_half, pulled_half))
    return (results[0].reshape(queries.shape), results[1].reshape(queries.shape), results[2].reshape(queries.shape), results[3].reshape(queries.shape))
```

```python
import functools
import math

import jax
import jax.numpy as jnp
from jax import lax
from jax.experimental import pallas as pl
from jax.experimental.pallas import tpu as pltpu
from jax.sharding import PartitionSpec as P

MESH = pl.DeviceIdType.MESH
F32 = jnp.float32
BF16 = jnp.bfloat16
NN = (((1,), (0,)), ((), ()))
NT = (((1,), (1,)), ((), ()))
TN = (((0,), (0,)), ((), ()))
CHUNK = 128
WIDE = 64
CUTS = (1, 2, 3, 6)


def mm(a, b, dims):
    return lax.dot_general(a, b, dims, preferred_element_type=F32)


def main_kernel(
    dims,
    q_hbm, k_hbm, v_hbm, g_hbm, tab_hbm, prof_hbm,
    lo_ref, lq_ref, lk_ref, lv_ref, wq_ref, wg_ref, bnt_ref, bnn_ref, pul_ref, k_ref, v_ref,
    q_ref, g_ref, tab_ref, prof_ref, in_sem,
    tbl_scr, w_scr, lev_scr, m_scr, p_scr, d_scr,
    s_scr, st, x0, pin, tots, far, ains, outs,
    pair_send, pair_recv, a_send, a_recv, b_send, b_recv, c_send, c_recv,
):
    T, H, D, cols, rows, span = dims
    chip_bits = rows.bit_length() - 2
    bits = chip_bits + cols.bit_length() - 1
    L = bits + 1
    top = L - 1
    tile_bits = T.bit_length() - 1
    span_bits = span.bit_length() - 1
    z = lax.axis_index("col")
    row = lax.axis_index("row")
    core = lax.rem(row, 2)
    chip = lax.div(row, 2)
    other = 1 - core
    digits = [lax.rem(lax.div(chip, 1 << i), 2) for i in range(chip_bits)]
    digits += [lax.rem(lax.div(z, 1 << i), 2) for i in range(bits - chip_bits)]
    upper = [core] + digits

    def flipped(flip, low, high):
        total = 0
        for i in range(low, high):
            digit = 1 - digits[i] if flip >> i & 1 else digits[i]
            total = total + digit * (1 << i - low)
        return total

    def device(flip, which):
        return (flipped(flip, chip_bits, bits), flipped(flip, 0, chip_bits) * 2 + which)

    loads = [
        pltpu.make_async_copy(src, dst, in_sem.at[n])
        for n, (src, dst) in enumerate(
            [(prof_hbm, prof_ref), (tab_hbm, tab_ref), (q_hbm, q_ref), (g_hbm, g_ref),
             (v_hbm, v_ref), (k_hbm, k_ref)]
        )
    ]
    for load in loads:
        load.start()
    half = 1 << top - 1
    barrier = pltpu.get_barrier_semaphore()
    greeted = [(flip, which) for flip in range(half) for which in (core, other)][1:]
    greeted.append((half, core))
    for flip, which in greeted:
        pl.semaphore_signal(barrier, inc=1, device_id=device(flip, which), device_id_type=MESH)

    def remote(src, dst, send, recv, to):
        return pltpu.make_async_remote_copy(
            src_ref=src, dst_ref=dst, send_sem=send, recv_sem=recv,
            device_id=to, device_id_type=MESH,
        )

    profiles = tab_ref.shape[2]
    levels = tab_ref.shape[0]
    tbl_scr[...] = jnp.zeros_like(tbl_scr)
    loads[0].wait()
    loads[1].wait()
    onehot = jnp.where(
        lax.broadcasted_iota(jnp.int32, (profiles, T), 0) == prof_ref[...], 1.0, 0.0
    ).astype(BF16)
    onehot = jnp.concatenate([onehot, onehot, onehot], axis=0)
    place = lax.broadcasted_iota(jnp.int32, (levels, profiles), 0)
    scale = jnp.zeros((levels, profiles), F32)
    for level in range(levels):
        scale = jnp.where(place == level, 2.0 ** (-0.5 * level) / math.sqrt(D), scale)
    for h in range(H):
        tbl_scr[:, h * WIDE : h * WIDE + levels] = jnp.transpose(tab_ref[:, h, :] * scale)
    table = tbl_scr[...]
    first = table.astype(BF16)
    rest = table - first.astype(F32)
    second = rest.astype(BF16)
    third = (rest - second.astype(F32)).astype(BF16)
    w_scr[...] = mm(onehot, jnp.concatenate([first, second, third], axis=0), TN)

    def column(h, rs, level):
        at = h * WIDE + level
        return w_scr[rs, at : at + 1]

    def weigh(src, dst, h, js):
        for start in range(0, T, CHUNK):
            rs = slice(start, start + CHUNK)
            x = src[rs, h * D : (h + 1) * D].astype(F32)
            for j in js:
                c = (h * L + j) * D
                dst[rs, c : c + D] = (x * column(h, rs, tile_bits + 1 + j)).astype(BF16)

    def heads(h):
        return slice(h * D, (h + 1) * D)

    loads[2].wait()
    for h in range(H):
        weigh(q_ref, wq_ref, h, [top])
    loads[3].wait()
    grads = [
        mm(g_ref[:, heads(h)], wq_ref[:, (h * L + top) * D : (h * L + L) * D], TN) for h in range(H)
    ]
    loads[4].wait()
    loads[5].wait()
    for h in range(H):
        s_scr[h] = mm(v_ref[:, heads(h)], k_ref[:, heads(h)], TN)
        st[top, h] = jnp.where(upper[top] == 1, grads[h], s_scr[h])

    def size(j):
        owners = min(1 << j - 1, D // 8)
        return 1 << j - 1, owners, D // owners

    def piece(index, R):
        return pl.ds(pl.multiple_of(index * R, R), R)

    direct = half <= D // 8

    def start_direct():
        n, owners, R = size(top)
        mine = flipped(0, 0, top - 1)
        for flip in range(n - 1, -1, -1):
            owner = flipped(flip, 0, top - 1)
            for which in (core, other):
                if flip == 0 and which is core:
                    continue
                remote(
                    st.at[top, which, piece(owner, R)], ains[top].at[mine * 2 + core],
                    a_send.at[top], a_recv.at[top], device(flip, which),
                ).start()
        ains[top][mine * 2 + core] = st[top, core, piece(mine, R), :]

    def start_reduce(j, source):
        n, owners, R = size(j)
        mine = flipped(0, 0, j - 1)
        for flip in range(n - 1, 0, -1):
            owner = flipped(flip, 0, j - 1)

            def send():
                remote(
                    source.at[piece(owner, R)], ains[j].at[mine],
                    a_send.at[j], a_recv.at[j], device(flip, core),
                ).start()

            if owners < n:
                pl.when(owner < owners)(send)
            else:
                send()
        if owners < n:
            @pl.when(mine < owners)
            def _():
                ains[j][mine] = source[piece(mine, R), :]
        else:
            ains[j][mine] = source[piece(mine, R), :]

    def spread(j):
        n, owners, R = size(j)
        mine = flipped(0, 0, j - 1)
        count = ains[j].shape[0]

        def go():
            if count > 1:
                got = ains[j].at[pl.ds(0, count - 1)]
                remote(got, got, a_send.at[j], a_recv.at[j], device(half, core)).wait_recv()
            outs[j][...] = sum([ains[j][p] for p in range(1, count)], ains[j][0])
            for flip in range(n, 2 * n):
                remote(
                    outs[j], far.at[j, core, piece(mine, R)],
                    b_send.at[j], b_recv.at[j], device(flip, core),
                ).start()

        if owners < n:
            pl.when(mine < owners)(go)
        else:
            go()

    def arrived(j):
        whole = far.at[j, core]
        remote(whole, whole, b_send.at[j], b_recv.at[j], device(half, core)).wait_recv()

    def settle(j):
        n, owners, R = size(j)
        mine = flipped(0, 0, j - 1)
        count = ains[j].shape[0]

        def sent(ref, sem):
            remote(ref, ref, sem, a_recv.at[j], device(half, core)).wait_send()

        if owners < n:
            for flip in range(n - 1, 0, -1):
                @pl.when(flipped(flip, 0, j - 1) < owners)
                def _():
                    sent(outs[j], a_send.at[j])

            @pl.when(mine < owners)
            def _():
                sent(ains[j], b_send.at[j])
        else:
            if count > 1:
                sent(ains[j].at[pl.ds(0, count - 1)], a_send.at[j])
            sent(ains[j].at[pl.ds(0, n)], b_send.at[j])

    pl.semaphore_wait(barrier, len(greeted))
    if direct:
        start_direct()
    for h in range(H):
        weigh(q_ref, wq_ref, h, range(top))
        low = mm(g_ref[:, heads(h)], wq_ref[:, h * L * D : (h * L + top) * D], TN)
        state = s_scr[h]
        for j in range(1, top):
            st[j, h] = jnp.where(upper[j] == 1, low[:, j * D : (j + 1) * D], state)
        x0[h] = jnp.where(core == 0, state, low[:, :D])
    partner = device(0, other)
    pooled = top if direct else L
    pair = remote(
        st.at[pl.ds(1, pooled - 1), other], pin, pair_send.at[0], pair_recv.at[0], partner
    )
    pair.start()
    near = remote(x0, far.at[0], pair_send.at[1], pair_recv.at[1], partner)
    near.start()

    r_at = lax.broadcasted_iota(jnp.int32, (span, span), 0)
    c_at = lax.broadcasted_iota(jnp.int32, (span, span), 1)
    apart = jnp.bitwise_xor(r_at, c_at)
    lev = jnp.zeros((span, span), jnp.int32)
    for bit in range(span_bits):
        lev = lev + jnp.where(apart >= 1 << bit, 1, 0)
    lev_scr[...] = jnp.where(c_at <= r_at, lev, -1)

    last = T // span - 1

    def unit(h, i):
        hs = heads(h)
        ts = slice(i * span, (i + 1) * span)
        width = (i + 1) * span
        for start in range(0, span, 64):
            rs = slice(start, start + 64)
            wts = slice(i * span + start, i * span + start + 64)
            mask = jnp.zeros((64, span), F32)
            here = lev_scr[rs, :]
            for level in range(span_bits + 1):
                mask = jnp.where(here == level, column(h, wts, level), mask)
            m_scr[rs, :] = mask
        q = q_ref[ts, hs]
        g = g_ref[ts, hs]
        for b in range(i + 1):
            bs = slice(b * span, (b + 1) * span)
            if b < i:
                mask = column(h, ts, span_bits + (b ^ i).bit_length())
            else:
                mask = m_scr[...]
            p_scr[:, bs] = (mm(q, k_ref[bs, hs], NT) * mask).astype(BF16)
            d_scr[:, bs] = (mm(g, v_ref[bs, hs], NT) * mask).astype(BF16)
        ws = slice(0, width)
        lo_ref[ts, hs] = mm(p_scr[:, ws], v_ref[ws, hs], NN)
        lq_ref[ts, hs] = mm(d_scr[:, ws], k_ref[ws, hs], NN)
        dk = mm(d_scr[:, ws], q, TN)
        dv = mm(p_scr[:, ws], g, TN)
        if i == last:
            lk_ref[ws, hs] = dk
            lv_ref[ws, hs] = dv
        else:
            lk_ref[ws, hs] += dk
            lv_ref[ws, hs] += dv

    work = [(h, i) for i in range(last, -1, -1) for h in range(H)]

    def units(start, end):
        for h, i in work[len(work) * start // 8 : len(work) * end // 8]:
            unit(h, i)

    units(0, CUTS[0])
    pair.wait()
    for j in range(pooled - 1, 0, -1):
        tots[j - 1] = st[j, core] + pin[j - 1]
        if j == 1:
            ains[1][0] = tots[0]
        else:
            start_reduce(j, tots.at[j - 1])
    spread(1)
    units(CUTS[0], CUTS[1])
    spread(top)
    units(CUTS[1], CUTS[2])
    for j in range(top - 1, 1, -1):
        spread(j)
    units(CUTS[2], CUTS[3])
    for h in range(H):
        weigh(g_ref, wg_ref, h, range(L))

    def relay(low, high, n):
        ref = far.at[pl.ds(low, high - low), core]
        copy = remote(ref, ref, c_send.at[n], c_recv.at[n], partner)
        copy.start()
        return copy

    for j in range(1, top):
        arrived(j)
    early = relay(1, top, 0)
    units(CUTS[3], 8)
    near.wait()
    early.wait_recv()

    def gather(h, js, pulled):
        for j in js:
            value = far[j, h]
            up = upper[j] == 1
            pulled = pulled + jnp.where(up, 0.0, value)
            chosen = jnp.where(up, value, 0.0).astype(BF16)
            bnt_ref[h, :, j * D : (j + 1) * D] = chosen
            bnn_ref[h, j * D : (j + 1) * D, :] = chosen
        return pulled

    for h in range(H):
        s_scr[h] = gather(h, range(top), jnp.zeros((D, D), F32))
    arrived(top)
    late = relay(top, L, 1)
    for j in range(1, L):
        settle(j)
    early.wait_send()
    late.wait()
    for h in range(H):
        pul_ref[h] = gather(h, [top], s_scr[h]).astype(BF16)


def finish_kernel(
    dims, lo, lq, lk, lv, wq, wg, k, v, bnt, bnn, pul, out, dq, dk, dv
):
    H, D, L, block = dims
    ts = pl.ds(pl.multiple_of(pl.program_id(0) * block, block), block)
    for h in range(H):
        hs = slice(h * D, (h + 1) * D)
        ls = slice(h * L * D, (h + 1) * L * D)
        out[:, hs] = lo[ts, hs] + mm(wq[ts, ls], bnt[h], NT)
        dq[:, hs] = lq[ts, hs] + mm(wg[ts, ls], bnn[h], NN)
        dk[:, hs] = lk[ts, hs] + mm(v[ts, hs], pul[h], NN)
        dv[:, hs] = lv[ts, hs] + mm(k[ts, hs], pul[h], NT)


def shards(cols, rows, queries, keys, values, out_grad, weight_table, profile):
    T = queries.shape[0]
    H = weight_table.shape[1]
    D = queries.shape[1] // H
    levels = weight_table.shape[2]
    L = rows.bit_length() + cols.bit_length() - 2
    profiles = weight_table.shape[0]
    top = L - 1
    direct = 1 << top - 1 <= D // 8
    span = min(T, 256)
    assert H == 2 and L > 2 and H * WIDE == 128 and levels <= WIDE
    pieces = [(8, D), (1, D, D)]
    for j in range(2, L):
        n = 1 << j - 1
        R = D // min(n, D // 8)
        pieces.append((n * (2 if direct and j == top else 1), R, D))
    vm = pl.BlockSpec(memory_space=pltpu.VMEM)
    sds = jax.ShapeDtypeStruct
    dma = pltpu.SemaphoreType.DMA
    local = sds((T, H * D), F32)
    weighted = sds((T, H * L * D), BF16)
    parts = pl.pallas_call(
        functools.partial(main_kernel, (T, H, D, cols, rows, span)),
        out_shape=[
            local, local, local, local, weighted, weighted,
            sds((H, D, L * D), BF16), sds((H, L * D, D), BF16), sds((H, D, D), BF16),
            sds((T, H * D), BF16), sds((T, H * D), BF16),
        ],
        in_specs=[pl.BlockSpec(memory_space=pltpu.HBM)] * 6,
        out_specs=[vm] * 11,
        scratch_shapes=[
            pltpu.VMEM((T, H * D), BF16),
            pltpu.VMEM((T, H * D), BF16),
            pltpu.VMEM((levels, H, profiles), F32),
            pltpu.VMEM((1, T), jnp.int32),
            dma((6,)),
            pltpu.VMEM((profiles, H * WIDE), F32),
            pltpu.VMEM((T, H * WIDE), F32),
            pltpu.VMEM((span, span), jnp.int32),
            pltpu.VMEM((span, span), F32),
            pltpu.VMEM((span, T), BF16),
            pltpu.VMEM((span, T), BF16),
            pltpu.VMEM((H, D, D), F32),
            pltpu.VMEM((L, H, D, D), F32),
            pltpu.VMEM((H, D, D), F32),
            pltpu.VMEM(((top if direct else L) - 1, D, D), F32),
            pltpu.VMEM(((top if direct else L) - 1, D, D), F32),
            pltpu.VMEM((L, H, D, D), F32),
            [pltpu.VMEM(shape, F32) for shape in pieces],
            [pltpu.VMEM(shape[-2:], F32) for shape in pieces],
            dma((2,)), dma((2,)),
            dma((L,)), dma((L,)),
            dma((L,)), dma((L,)),
            dma((2,)), dma((2,)),
        ],
        compiler_params=pltpu.CompilerParams(
            collective_id=0, has_side_effects=True, vmem_limit_bytes=40 * 1024 * 1024
        ),
        name="main",
    )(*[pltpu.with_memory_space_constraint(a, pltpu.HBM) for a in (queries, keys, values, out_grad, jnp.transpose(weight_table, (2, 1, 0)), profile.reshape(1, T))])
    lo, lq, lk, lv, wq, wg, bnt, bnn, pul, k_near, v_near = parts
    block = min(T, 256)
    tile = pl.BlockSpec((block, H * D), lambda i: (i, 0))
    return pl.pallas_call(
        functools.partial(finish_kernel, (H, D, L, block)),
        grid=(T // block,),
        out_shape=[local] * 4,
        in_specs=[vm] * 11,
        out_specs=[tile] * 4,
        compiler_params=pltpu.CompilerParams(vmem_limit_bytes=24 * 1024 * 1024),
        name="finish",
    )(lo, lq, lk, lv, wq, wg, k_near, v_near, bnt, bnn, pul)


def solution(mesh):
    tokens = P(("col", "row"), None)
    return jax.shard_map(
        functools.partial(shards, mesh.shape["col"], mesh.shape["row"]),
        mesh=mesh,
        in_specs=(tokens,) * 4 + (P(), P(("col", "row"))),
        out_specs=(tokens,) * 4,
        check_vma=False,
    )
```

```python
import functools
import math

import jax
import jax.numpy as jnp
from jax import lax
from jax.experimental import pallas as pl
from jax.experimental.pallas import tpu as pltpu
from jax.sharding import PartitionSpec as P

MESH = pl.DeviceIdType.MESH
F32 = jnp.float32
BF16 = jnp.bfloat16
NN = (((1,), (0,)), ((), ()))
NT = (((1,), (1,)), ((), ()))
TN = (((0,), (0,)), ((), ()))
CHUNK = 128
WIDE = 64
CUTS = (1, 2, 2, 6)
SPAN = 256
FLAT, DIRECT, POOLED = range(3)


def level_kinds(L, D):
    kinds = [None]
    for j in range(1, L):
        n = 1 << j - 1
        kinds.append(FLAT if n <= 2 and j < L - 1 else DIRECT if n <= D // 16 else POOLED)
    for j in range(1, L):
        if any(kind != DIRECT for kind in kinds[j:]) and kinds[j] == DIRECT:
            kinds[j] = POOLED
    return kinds


def mm(a, b, dims):
    return lax.dot_general(a, b, dims, preferred_element_type=F32)


def main_kernel(
    dims,
    q_hbm, k_hbm, v_hbm, g_hbm, tab_hbm, prof_hbm,
    lo_ref, lq_ref, lk_ref, lv_ref, wq_ref, wg_ref, bnt_ref, bnn_ref, pul_ref, bl_ref, k_ref, v_ref,
    q_ref, g_ref, tab_ref, prof_ref, in_sem,
    tbl_scr, w_scr, lev_scr, gt_scr, p_scr, d_scr,
    s_scr, pl_scr, st, x0, pin, tots, far, ains, outs,
    pair_send, pair_recv, a_send, a_recv, b_send, b_recv, c_send, c_recv,
):
    T, H, D, cols, rows, span = dims
    chip_bits = rows.bit_length() - 2
    bits = chip_bits + cols.bit_length() - 1
    L = bits + 1
    top = L - 1
    tile_bits = T.bit_length() - 1
    span_bits = span.bit_length() - 1
    blocks = T // span
    LB = blocks.bit_length() - 1
    K = L + LB
    z = lax.axis_index("col")
    row = lax.axis_index("row")
    core = lax.rem(row, 2)
    chip = lax.div(row, 2)
    other = 1 - core
    digits = [lax.rem(lax.div(chip, 1 << i), 2) for i in range(chip_bits)]
    digits += [lax.rem(lax.div(z, 1 << i), 2) for i in range(bits - chip_bits)]
    upper = [core] + digits

    def flipped(flip, low, high):
        total = 0
        for i in range(low, high):
            digit = 1 - digits[i] if flip >> i & 1 else digits[i]
            total = total + digit * (1 << i - low)
        return total

    def device(flip, which):
        return (flipped(flip, chip_bits, bits), flipped(flip, 0, chip_bits) * 2 + which)

    loads = [
        pltpu.make_async_copy(src, dst, in_sem.at[n])
        for n, (src, dst) in enumerate(
            [(prof_hbm, prof_ref), (tab_hbm, tab_ref), (q_hbm, q_ref), (g_hbm, g_ref),
             (v_hbm, v_ref), (k_hbm, k_ref)]
        )
    ]
    for load in loads:
        load.start()
    half = 1 << top - 1
    barrier = pltpu.get_barrier_semaphore()
    greeted = [(flip, which) for flip in range(half) for which in (core, other)][1:]
    greeted.append((half, core))
    for flip, which in greeted:
        pl.semaphore_signal(barrier, inc=1, device_id=device(flip, which), device_id_type=MESH)

    def remote(src, dst, send, recv, to):
        return pltpu.make_async_remote_copy(
            src_ref=src, dst_ref=dst, send_sem=send, recv_sem=recv,
            device_id=to, device_id_type=MESH,
        )

    profiles = tab_ref.shape[2]
    levels = tab_ref.shape[0]
    tbl_scr[...] = jnp.zeros_like(tbl_scr)
    loads[0].wait()
    loads[1].wait()
    onehot = jnp.where(
        lax.broadcasted_iota(jnp.int32, (profiles, T), 0) == prof_ref[...], 1.0, 0.0
    ).astype(BF16)
    onehot = jnp.concatenate([onehot, onehot, onehot], axis=0)
    place = lax.broadcasted_iota(jnp.int32, (levels, profiles), 0)
    scale = jnp.zeros((levels, profiles), F32)
    for level in range(levels):
        scale = jnp.where(place == level, 2.0 ** (-0.5 * level) / math.sqrt(D), scale)
    for h in range(H):
        tbl_scr[:, h * WIDE : h * WIDE + levels] = jnp.transpose(tab_ref[:, h, :] * scale)
    table = tbl_scr[...]
    first = table.astype(BF16)
    rest = table - first.astype(F32)
    second = rest.astype(BF16)
    third = (rest - second.astype(F32)).astype(BF16)
    w_scr[...] = mm(onehot, jnp.concatenate([first, second, third], axis=0), TN)

    def column(h, rs, level):
        at = h * WIDE + level
        return w_scr[rs, at : at + 1]

    def weigh(src, dst, h, js):
        for start in range(0, T, CHUNK):
            rs = slice(start, start + CHUNK)
            x = src[rs, h * D : (h + 1) * D].astype(F32)
            for j in js:
                c = (h * K + j) * D
                dst[rs, c : c + D] = (x * column(h, rs, tile_bits + 1 + j)).astype(BF16)

    def weighed(h, low, high):
        return wq_ref[:, (h * K + low) * D : (h * K + high) * D]

    def heads(h):
        return slice(h * D, (h + 1) * D)

    loads[2].wait()
    for h in range(H):
        weigh(q_ref, wq_ref, h, [top])
    loads[3].wait()
    for h in range(H):
        gt_scr[h] = jnp.transpose(g_ref[:, heads(h)])
    grads = [mm(gt_scr[h], weighed(h, top, L), NN) for h in range(H)]
    loads[4].wait()
    loads[5].wait()
    for h in range(H):
        parts = []
        for i in range(blocks):
            ts = slice(i * span, (i + 1) * span)
            parts.append(mm(v_ref[ts, heads(h)], k_ref[ts, heads(h)], TN))
        at = 0
        for m in range(LB):
            for group in range(0, len(parts), 2):
                bl_ref[h, at] = parts[group].astype(BF16)
                at += 1
            parts = [parts[group] + parts[group + 1] for group in range(0, len(parts), 2)]
        s_scr[h] = parts[0]
        st[top, h] = jnp.where(upper[top] == 1, grads[h], s_scr[h])

    def size(j):
        owners = min(1 << j - 1, D // 8)
        return 1 << j - 1, owners, D // owners

    def piece(index, R):
        return pl.ds(pl.multiple_of(index * R, R), R)

    kinds = level_kinds(L, D)

    def start_direct(j):
        n, owners, R = size(j)
        mine = flipped(0, 0, j - 1)
        for flip in range(n - 1, -1, -1):
            owner = flipped(flip, 0, j - 1)
            for which in (core, other):
                if flip == 0 and which is core:
                    continue
                remote(
                    st.at[j, which, piece(owner, R)], ains[j].at[mine * 2 + core],
                    a_send.at[j], a_recv.at[j], device(flip, which),
                ).start()
        ains[j][mine * 2 + core] = st[j, core, piece(mine, R), :]

    def start_flat(j, source):
        n = 1 << j - 1
        slot = ains[j].at[flipped(0, 0, j - 1)] if n > 1 else far.at[j, core]
        for flip in range(n, 2 * n):
            remote(source, slot, b_send.at[j], b_recv.at[j], device(flip, core)).start()

    def start_reduce(j, source):
        n, owners, R = size(j)
        mine = flipped(0, 0, j - 1)
        for flip in range(n - 1, 0, -1):
            owner = flipped(flip, 0, j - 1)

            def send():
                remote(
                    source.at[piece(owner, R)], ains[j].at[mine],
                    a_send.at[j], a_recv.at[j], device(flip, core),
                ).start()

            if owners < n:
                pl.when(owner < owners)(send)
            else:
                send()
        if owners < n:
            @pl.when(mine < owners)
            def _():
                ains[j][mine] = source[piece(mine, R), :]
        else:
            ains[j][mine] = source[piece(mine, R), :]

    def spread(j):
        n, owners, R = size(j)
        mine = flipped(0, 0, j - 1)
        count = ains[j].shape[0]

        def go():
            if count > 1:
                got = ains[j].at[pl.ds(0, count - 1)]
                remote(got, got, a_send.at[j], a_recv.at[j], device(half, core)).wait_recv()
            outs[j][...] = sum([ains[j][p] for p in range(1, count)], ains[j][0])
            for flip in range(n, 2 * n):
                remote(
                    outs[j], far.at[j, core, piece(mine, R)],
                    b_send.at[j], b_recv.at[j], device(flip, core),
                ).start()

        if owners < n:
            pl.when(mine < owners)(go)
        else:
            go()

    def arrived(j):
        flat = kinds[j] == FLAT and j > 1
        whole = ains[j] if flat else far.at[j, core]
        remote(whole, whole, b_send.at[j], b_recv.at[j], device(half, core)).wait_recv()
        if flat:
            far[j, core] = sum([ains[j][p] for p in range(1, 1 << j - 1)], ains[j][0])

    def settle(j):
        n, owners, R = size(j)
        mine = flipped(0, 0, j - 1)
        count = ains[j].shape[0]

        def sent(ref, sem):
            remote(ref, ref, sem, a_recv.at[j], device(half, core)).wait_send()

        if kinds[j] == FLAT:
            sent(ains[j], b_send.at[j])
        elif owners < n:
            for flip in range(n - 1, 0, -1):
                @pl.when(flipped(flip, 0, j - 1) < owners)
                def _():
                    sent(outs[j], a_send.at[j])

            @pl.when(mine < owners)
            def _():
                sent(ains[j], b_send.at[j])
        else:
            if count > 1:
                sent(ains[j].at[pl.ds(0, count - 1)], a_send.at[j])
            sent(ains[j].at[pl.ds(0, n)], b_send.at[j])

    pl.semaphore_wait(barrier, len(greeted))
    if kinds[top] == DIRECT:
        start_direct(top)
    done = top
    if kinds[top - 1] == DIRECT:
        done = top - 1
        for h in range(H):
            weigh(q_ref, wq_ref, h, [done])
            high = mm(gt_scr[h], weighed(h, done, top), NN)
            st[done, h] = jnp.where(upper[done] == 1, high, s_scr[h])
        start_direct(done)
    for h in range(H):
        weigh(q_ref, wq_ref, h, range(done))
        low = mm(gt_scr[h], weighed(h, 0, done), NN)
        state = s_scr[h]
        for j in range(1, done):
            st[j, h] = jnp.where(upper[j] == 1, low[:, j * D : (j + 1) * D], state)
        x0[h] = jnp.where(core == 0, state, low[:, :D])
    partner = device(0, other)
    pooled = min([j for j in range(1, L) if kinds[j] == DIRECT], default=L)
    pair = remote(
        st.at[pl.ds(1, pooled - 1), other], pin, pair_send.at[0], pair_recv.at[0], partner
    )
    pair.start()
    near = remote(x0, far.at[0], pair_send.at[1], pair_recv.at[1], partner)
    near.start()

    r_at = lax.broadcasted_iota(jnp.int32, (span, span), 0)
    c_at = lax.broadcasted_iota(jnp.int32, (span, span), 1)
    apart = jnp.bitwise_xor(r_at, c_at)
    lev = jnp.zeros((span, span), jnp.int32)
    for bit in range(span_bits):
        lev = lev + jnp.where(apart >= 1 << bit, 1, 0)
    lev_scr[...] = jnp.where(c_at <= r_at, lev, -1)

    def local_states(h):
        for i in range(1, blocks):
            for start in range(i * span, (i + 1) * span, CHUNK):
                rs = slice(start, start + CHUNK)
                xq = q_ref[rs, heads(h)].astype(F32)
                xg = g_ref[rs, heads(h)].astype(F32)
                for m in range(LB):
                    if i >> m & 1:
                        c = (h * K + L + m) * D
                        w = column(h, rs, span_bits + 1 + m)
                        wq_ref[rs, c : c + D] = (xq * w).astype(BF16)
                        wg_ref[rs, c : c + D] = (xg * w).astype(BF16)
        pulls = [None] * blocks
        for m in range(LB):
            step = 1 << m
            c = (h * K + L + m) * D
            for low in range(0, blocks, 2 * step):
                rs = slice((low + step) * span, (low + 2 * step) * span)
                grad = mm(gt_scr[h, :, rs], wq_ref[rs, c : c + D], NN)
                for i in range(low, low + step):
                    pulls[i] = grad if pulls[i] is None else pulls[i] + grad
        for i in range(blocks):
            pl_scr[i, h] = jnp.zeros((D, D), F32) if pulls[i] is None else pulls[i]

    def unit(h, i):
        hs = heads(h)
        ts = slice(i * span, (i + 1) * span)
        q, k, v, g = q_ref[ts, hs], k_ref[ts, hs], v_ref[ts, hs], g_ref[ts, hs]
        scores = mm(q, k, NT)
        grad_scores = mm(g, v, NT)
        for start in range(0, span, 64):
            rs = slice(start, start + 64)
            wts = slice(i * span + start, i * span + start + 64)
            mask = jnp.zeros((64, span), F32)
            here = lev_scr[rs, :]
            for level in range(span_bits + 1):
                mask = jnp.where(here == level, column(h, wts, level), mask)
            p_scr[rs, :] = (scores[rs, :] * mask).astype(BF16)
            d_scr[rs, :] = (grad_scores[rs, :] * mask).astype(BF16)
        lo_ref[ts, hs] = mm(p_scr[...], v, NN)
        lq_ref[ts, hs] = mm(d_scr[...], k, NN)
        lk_ref[ts, hs] = mm(d_scr[...], q, TN)
        lv_ref[ts, hs] = mm(p_scr[...], g, TN)

    work = [(h, i) for i in range(blocks) for h in range(H)]

    def units(start, end):
        for h, i in work[len(work) * start // 8 : len(work) * end // 8]:
            unit(h, i)

    units(0, CUTS[0])
    pair.wait()
    for j in range(pooled - 1, 0, -1):
        tots[j - 1] = st[j, core] + pin[j - 1]
        if kinds[j] == FLAT:
            start_flat(j, tots.at[j - 1])
        else:
            start_reduce(j, tots.at[j - 1])
    spreads = [j for j in range(top, 0, -1) if kinds[j] != FLAT]
    units(CUTS[0], CUTS[1])
    spread(spreads[0])
    units(CUTS[1], CUTS[2])
    for j in spreads[1:]:
        spread(j)
    units(CUTS[2], CUTS[3])
    def relay(low, high, n):
        ref = far.at[pl.ds(low, high - low), core]
        copy = remote(ref, ref, c_send.at[n], c_recv.at[n], partner)
        copy.start()
        return copy

    flats = [j for j in range(1, L) if kinds[j] == FLAT]
    near.wait()
    for j in flats:
        arrived(j)
    early = relay(1, 1 + len(flats), 0)
    for h in range(H):
        weigh(g_ref, wg_ref, h, range(L))
    units(CUTS[3], 8)
    for h in range(H):
        local_states(h)
    for j in range(1 + len(flats), top):
        arrived(j)
    middle = relay(1 + len(flats), top, 2)
    early.wait()

    def gather(h, js, pulled):
        for j in js:
            value = far[j, h]
            up = upper[j] == 1
            pulled = pulled + jnp.where(up, 0.0, value)
            chosen = jnp.where(up, value, 0.0).astype(BF16)
            bnt_ref[h, :, j * D : (j + 1) * D] = chosen
            bnn_ref[h, j * D : (j + 1) * D, :] = chosen
        return pulled

    split = 1 + len(flats)
    for h in range(H):
        s_scr[h] = gather(h, range(split), jnp.zeros((D, D), F32))
    middle.wait()
    for h in range(H):
        s_scr[h] = gather(h, range(split, top), s_scr[h])
    arrived(top)
    late = relay(top, L, 1)
    for j in range(1, L):
        settle(j)
    late.wait()
    for h in range(H):
        pulled = gather(h, [top], s_scr[h])
        for i in range(blocks):
            pul_ref[i, h] = (pulled + pl_scr[i, h]).astype(BF16)


def finish_kernel(
    dims, lo, lq, lk, lv, wq, wg, k, v, bnt, bnn, pul, bl,
    out_hbm, dq_hbm, dk_hbm, dv_hbm, out, dq, dk, dv, sem,
):
    H, D, L, span = dims
    blocks = lo.shape[0] // span
    LB = blocks.bit_length() - 1
    K = L + LB
    copies = []
    for i in range(blocks):
        ts = slice(i * span, (i + 1) * span)
        for h in range(H):
            hs = slice(h * D, (h + 1) * D)
            dk[ts, hs] = lk[ts, hs] + mm(v[ts, hs], pul[i, h], NN)
            dv[ts, hs] = lv[ts, hs] + mm(k[ts, hs], pul[i, h], NT)
            ls = slice(h * K * D, (h * K + L) * D)
            o = lo[ts, hs] + mm(wq[ts, ls], bnt[h], NT)
            b = lq[ts, hs] + mm(wg[ts, ls], bnn[h], NN)
            at = 0
            for m in range(LB):
                if i >> m & 1:
                    c = (h * K + L + m) * D
                    state = bl[h, at + (i >> m + 1)]
                    o = o + mm(wq[ts, c : c + D], state, NT)
                    b = b + mm(wg[ts, c : c + D], state, NN)
                at += blocks >> m + 1
            out[ts, hs] = o
            dq[ts, hs] = b
        for n, (src, dst) in enumerate(
            [(dk, dk_hbm), (dv, dv_hbm), (out, out_hbm), (dq, dq_hbm)]
        ):
            copy = pltpu.make_async_copy(src.at[ts], dst.at[ts], sem.at[i, n])
            copy.start()
            copies.append(copy)
    for copy in copies:
        copy.wait()


def shards(cols, rows, queries, keys, values, out_grad, weight_table, profile):
    T = queries.shape[0]
    H = weight_table.shape[1]
    D = queries.shape[1] // H
    levels = weight_table.shape[2]
    L = rows.bit_length() + cols.bit_length() - 2
    profiles = weight_table.shape[0]
    top = L - 1
    kinds = level_kinds(L, D)
    pooled = min([j for j in range(1, L) if kinds[j] == DIRECT], default=L)
    span = min(T, SPAN)
    blocks = T // span
    LB = blocks.bit_length() - 1
    assert H == 2 and L > 2 and H * WIDE == 128 and levels <= WIDE
    pieces = [(8, D)]
    for j in range(1, L):
        n = 1 << j - 1
        R = D if kinds[j] == FLAT else D // min(n, D // 8)
        pieces.append((n * (2 if kinds[j] == DIRECT else 1), R, D))
    vm = pl.BlockSpec(memory_space=pltpu.VMEM)
    sds = jax.ShapeDtypeStruct
    dma = pltpu.SemaphoreType.DMA
    local = sds((T, H * D), F32)
    weighted = sds((T, H * (L + LB) * D), BF16)
    parts = pl.pallas_call(
        functools.partial(main_kernel, (T, H, D, cols, rows, span)),
        out_shape=[
            local, local, local, local, weighted, weighted,
            sds((H, D, L * D), BF16), sds((H, L * D, D), BF16), sds((blocks, H, D, D), BF16),
            sds((H, max(blocks - 1, 1), D, D), BF16),
            sds((T, H * D), BF16), sds((T, H * D), BF16),
        ],
        in_specs=[pl.BlockSpec(memory_space=pltpu.HBM)] * 6,
        out_specs=[vm] * 12,
        scratch_shapes=[
            pltpu.VMEM((T, H * D), BF16),
            pltpu.VMEM((T, H * D), BF16),
            pltpu.VMEM((levels, H, profiles), F32),
            pltpu.VMEM((1, T), jnp.int32),
            dma((6,)),
            pltpu.VMEM((profiles, H * WIDE), F32),
            pltpu.VMEM((T, H * WIDE), F32),
            pltpu.VMEM((span, span), jnp.int32),
            pltpu.VMEM((H, D, T), BF16),
            pltpu.VMEM((span, span), BF16),
            pltpu.VMEM((span, span), BF16),
            pltpu.VMEM((H, D, D), F32),
            pltpu.VMEM((blocks, H, D, D), F32),
            pltpu.VMEM((L, H, D, D), F32),
            pltpu.VMEM((H, D, D), F32),
            pltpu.VMEM((pooled - 1, D, D), F32),
            pltpu.VMEM((pooled - 1, D, D), F32),
            pltpu.VMEM((L, H, D, D), F32),
            [pltpu.VMEM(shape, F32) for shape in pieces],
            [pltpu.VMEM(shape[-2:], F32) for shape in pieces],
            dma((2,)), dma((2,)),
            dma((L,)), dma((L,)),
            dma((L,)), dma((L,)),
            dma((3,)), dma((3,)),
        ],
        compiler_params=pltpu.CompilerParams(
            collective_id=0, has_side_effects=True, vmem_limit_bytes=40 * 1024 * 1024
        ),
        name="main",
    )(*[pltpu.with_memory_space_constraint(a, pltpu.HBM) for a in (queries, keys, values, out_grad, jnp.transpose(weight_table, (2, 1, 0)), profile.reshape(1, T))])
    lo, lq, lk, lv, wq, wg, bnt, bnn, pul, bl, k_near, v_near = parts
    return pl.pallas_call(
        functools.partial(finish_kernel, (H, D, L, span)),
        out_shape=[local] * 4,
        in_specs=[vm] * 12,
        out_specs=[pl.BlockSpec(memory_space=pltpu.HBM)] * 4,
        scratch_shapes=[pltpu.VMEM((T, H * D), F32)] * 4 + [dma((blocks, 4))],
        compiler_params=pltpu.CompilerParams(vmem_limit_bytes=24 * 1024 * 1024),
        name="finish",
    )(lo, lq, lk, lv, wq, wg, k_near, v_near, bnt, bnn, pul, bl)


def solution(mesh):
    tokens = P(("col", "row"), None)
    return jax.shard_map(
        functools.partial(shards, mesh.shape["col"], mesh.shape["row"]),
        mesh=mesh,
        in_specs=(tokens,) * 4 + (P(), P(("col", "row"))),
        out_specs=(tokens,) * 4,
        check_vma=False,
    )
```

```python
import functools
import math

import jax
import jax.numpy as jnp
from jax import lax
from jax.experimental import pallas as pl
from jax.experimental.pallas import tpu as pltpu
from jax.sharding import PartitionSpec as P

MESH = pl.DeviceIdType.MESH
F32 = jnp.float32
BF16 = jnp.bfloat16
NN = (((1,), (0,)), ((), ()))
NT = (((1,), (1,)), ((), ()))
TN = (((0,), (0,)), ((), ()))
CHUNK = 128
WIDE = 64
CUTS = (1, 2, 3, 7)
SPAN = 256
FLAT, DIRECT, POOLED = range(3)


def level_kinds(L, D):
    kinds = [None]
    for j in range(1, L):
        n = 1 << j - 1
        kinds.append(FLAT if n <= 2 and j < L - 1 else DIRECT if n <= D // 16 else POOLED)
    for j in range(1, L):
        if any(kind != DIRECT for kind in kinds[j:]) and kinds[j] == DIRECT:
            kinds[j] = POOLED
    return kinds


def mm(a, b, dims):
    return lax.dot_general(a, b, dims, preferred_element_type=F32)


def main_kernel(
    dims,
    q_hbm, k_hbm, v_hbm, g_hbm, tab_hbm, prof_hbm,
    lo_ref, lq_ref, lk_ref, lv_ref, wq_ref, wg_ref, bnt_ref, bnn_ref, pul_ref, bl_ref, k_ref, v_ref,
    q_ref, g_ref, tab_ref, prof_ref, in_sem,
    tbl_scr, w_scr, lev_scr, gt_scr, p_scr, d_scr,
    s_scr, pl_scr, st, x0, pin, tots, far, ains, outs,
    pair_send, pair_recv, a_send, a_recv, b_send, b_recv, c_send, c_recv,
):
    T, H, D, cols, rows, span = dims
    chip_bits = rows.bit_length() - 2
    bits = chip_bits + cols.bit_length() - 1
    L = bits + 1
    top = L - 1
    tile_bits = T.bit_length() - 1
    span_bits = span.bit_length() - 1
    blocks = T // span
    LB = blocks.bit_length() - 1
    K = L + LB
    z = lax.axis_index("col")
    row = lax.axis_index("row")
    core = lax.rem(row, 2)
    chip = lax.div(row, 2)
    other = 1 - core
    digits = [lax.rem(lax.div(chip, 1 << i), 2) for i in range(chip_bits)]
    digits += [lax.rem(lax.div(z, 1 << i), 2) for i in range(bits - chip_bits)]
    upper = [core] + digits

    def flipped(flip, low, high):
        total = 0
        for i in range(low, high):
            digit = 1 - digits[i] if flip >> i & 1 else digits[i]
            total = total + digit * (1 << i - low)
        return total

    def device(flip, which):
        return (flipped(flip, chip_bits, bits), flipped(flip, 0, chip_bits) * 2 + which)

    loads = [
        pltpu.make_async_copy(src, dst, in_sem.at[n])
        for n, (src, dst) in enumerate(
            [(prof_hbm, prof_ref), (tab_hbm, tab_ref), (q_hbm, q_ref), (g_hbm, g_ref),
             (v_hbm, v_ref), (k_hbm, k_ref)]
        )
    ]
    for load in loads:
        load.start()
    half = 1 << top - 1
    barrier = pltpu.get_barrier_semaphore()
    greeted = [(flip, which) for flip in range(half) for which in (core, other)][1:]
    greeted.append((half, core))
    for flip, which in greeted:
        pl.semaphore_signal(barrier, inc=1, device_id=device(flip, which), device_id_type=MESH)

    def remote(src, dst, send, recv, to):
        return pltpu.make_async_remote_copy(
            src_ref=src, dst_ref=dst, send_sem=send, recv_sem=recv,
            device_id=to, device_id_type=MESH,
        )

    profiles = tab_ref.shape[2]
    levels = tab_ref.shape[0]
    tbl_scr[...] = jnp.zeros_like(tbl_scr)
    loads[0].wait()
    loads[1].wait()
    onehot = jnp.where(
        lax.broadcasted_iota(jnp.int32, (profiles, T), 0) == prof_ref[...], 1.0, 0.0
    ).astype(BF16)
    onehot = jnp.concatenate([onehot, onehot, onehot], axis=0)
    place = lax.broadcasted_iota(jnp.int32, (levels, profiles), 0)
    scale = jnp.zeros((levels, profiles), F32)
    for level in range(levels):
        scale = jnp.where(place == level, 2.0 ** (-0.5 * level) / math.sqrt(D), scale)
    for h in range(H):
        tbl_scr[:, h * WIDE : h * WIDE + levels] = jnp.transpose(tab_ref[:, h, :] * scale)
    table = tbl_scr[...]
    first = table.astype(BF16)
    rest = table - first.astype(F32)
    second = rest.astype(BF16)
    third = (rest - second.astype(F32)).astype(BF16)
    w_scr[...] = mm(onehot, jnp.concatenate([first, second, third], axis=0), TN)

    def column(h, rs, level):
        at = h * WIDE + level
        return w_scr[rs, at : at + 1]

    def weigh(src, dst, h, js):
        for start in range(0, T, CHUNK):
            rs = slice(start, start + CHUNK)
            x = src[rs, h * D : (h + 1) * D].astype(F32)
            for j in js:
                c = (h * K + j) * D
                dst[rs, c : c + D] = (x * column(h, rs, tile_bits + 1 + j)).astype(BF16)

    def weighed(h, low, high):
        return wq_ref[:, (h * K + low) * D : (h * K + high) * D]

    def heads(h):
        return slice(h * D, (h + 1) * D)

    loads[2].wait()
    for h in range(H):
        weigh(q_ref, wq_ref, h, [top])
    loads[3].wait()
    for h in range(H):
        gt_scr[h] = jnp.transpose(g_ref[:, heads(h)])
    grads = [mm(gt_scr[h], weighed(h, top, L), NN) for h in range(H)]
    loads[4].wait()
    loads[5].wait()
    for h in range(H):
        parts = []
        for i in range(blocks):
            ts = slice(i * span, (i + 1) * span)
            parts.append(mm(v_ref[ts, heads(h)], k_ref[ts, heads(h)], TN))
        at = 0
        for m in range(LB):
            for group in range(0, len(parts), 2):
                bl_ref[h, at] = parts[group].astype(BF16)
                at += 1
            parts = [parts[group] + parts[group + 1] for group in range(0, len(parts), 2)]
        s_scr[h] = parts[0]
        st[top, h] = jnp.where(upper[top] == 1, grads[h], s_scr[h])

    def size(j):
        owners = min(1 << j - 1, D // 8)
        return 1 << j - 1, owners, D // owners

    def piece(index, R):
        return pl.ds(pl.multiple_of(index * R, R), R)

    kinds = level_kinds(L, D)

    def start_direct(j):
        n, owners, R = size(j)
        mine = flipped(0, 0, j - 1)
        for flip in range(n - 1, -1, -1):
            owner = flipped(flip, 0, j - 1)
            for which in (core, other):
                if flip == 0 and which is core:
                    continue
                remote(
                    st.at[j, which, piece(owner, R)], ains[j].at[mine * 2 + core],
                    a_send.at[j], a_recv.at[j], device(flip, which),
                ).start()
        ains[j][mine * 2 + core] = st[j, core, piece(mine, R), :]

    def start_flat(j, source):
        n = 1 << j - 1
        slot = ains[j].at[flipped(0, 0, j - 1)] if n > 1 else far.at[j, core]
        for flip in range(n, 2 * n):
            remote(source, slot, b_send.at[j], b_recv.at[j], device(flip, core)).start()

    def start_reduce(j, source):
        n, owners, R = size(j)
        mine = flipped(0, 0, j - 1)
        for flip in range(n - 1, 0, -1):
            owner = flipped(flip, 0, j - 1)

            def send():
                remote(
                    source.at[piece(owner, R)], ains[j].at[mine],
                    a_send.at[j], a_recv.at[j], device(flip, core),
                ).start()

            if owners < n:
                pl.when(owner < owners)(send)
            else:
                send()
        if owners < n:
            @pl.when(mine < owners)
            def _():
                ains[j][mine] = source[piece(mine, R), :]
        else:
            ains[j][mine] = source[piece(mine, R), :]

    def spread(j):
        n, owners, R = size(j)
        mine = flipped(0, 0, j - 1)
        count = ains[j].shape[0]

        def go():
            if count > 1:
                got = ains[j].at[pl.ds(0, count - 1)]
                remote(got, got, a_send.at[j], a_recv.at[j], device(half, core)).wait_recv()
            outs[j][...] = sum([ains[j][p] for p in range(1, count)], ains[j][0])
            for flip in range(n, 2 * n):
                remote(
                    outs[j], far.at[j, core, piece(mine, R)],
                    b_send.at[j], b_recv.at[j], device(flip, core),
                ).start()

        if owners < n:
            pl.when(mine < owners)(go)
        else:
            go()

    def arrived(j):
        flat = kinds[j] == FLAT and j > 1
        whole = ains[j] if flat else far.at[j, core]
        remote(whole, whole, b_send.at[j], b_recv.at[j], device(half, core)).wait_recv()
        if flat:
            far[j, core] = sum([ains[j][p] for p in range(1, 1 << j - 1)], ains[j][0])

    def settle(j):
        n, owners, R = size(j)
        mine = flipped(0, 0, j - 1)
        count = ains[j].shape[0]

        def sent(ref, sem):
            remote(ref, ref, sem, a_recv.at[j], device(half, core)).wait_send()

        if kinds[j] == FLAT:
            sent(ains[j], b_send.at[j])
        elif owners < n:
            for flip in range(n - 1, 0, -1):
                @pl.when(flipped(flip, 0, j - 1) < owners)
                def _():
                    sent(outs[j], a_send.at[j])

            @pl.when(mine < owners)
            def _():
                sent(ains[j], b_send.at[j])
        else:
            if count > 1:
                sent(ains[j].at[pl.ds(0, count - 1)], a_send.at[j])
            sent(ains[j].at[pl.ds(0, n)], b_send.at[j])

    pl.semaphore_wait(barrier, len(greeted))
    if kinds[top] == DIRECT:
        start_direct(top)
    done = top
    if kinds[top - 1] == DIRECT:
        done = top - 1
        for h in range(H):
            weigh(q_ref, wq_ref, h, [done])
            high = mm(gt_scr[h], weighed(h, done, top), NN)
            st[done, h] = jnp.where(upper[done] == 1, high, s_scr[h])
        start_direct(done)
    for h in range(H):
        weigh(q_ref, wq_ref, h, range(done))
        low = mm(gt_scr[h], weighed(h, 0, done), NN)
        state = s_scr[h]
        for j in range(1, done):
            st[j, h] = jnp.where(upper[j] == 1, low[:, j * D : (j + 1) * D], state)
        x0[h] = jnp.where(core == 0, state, low[:, :D])
    partner = device(0, other)
    pooled = min([j for j in range(1, L) if kinds[j] == DIRECT], default=L)
    pair = remote(
        st.at[pl.ds(1, pooled - 1), other], pin, pair_send.at[0], pair_recv.at[0], partner
    )
    pair.start()
    near = remote(x0, far.at[0], pair_send.at[1], pair_recv.at[1], partner)
    near.start()

    r_at = lax.broadcasted_iota(jnp.int32, (span, span), 0)
    c_at = lax.broadcasted_iota(jnp.int32, (span, span), 1)
    apart = jnp.bitwise_xor(r_at, c_at)
    lev = jnp.zeros((span, span), jnp.int32)
    for bit in range(span_bits):
        lev = lev + jnp.where(apart >= 1 << bit, 1, 0)
    lev_scr[...] = jnp.where(c_at <= r_at, lev, -1)

    def local_states(h):
        for i in range(1, blocks):
            for start in range(i * span, (i + 1) * span, CHUNK):
                rs = slice(start, start + CHUNK)
                xq = q_ref[rs, heads(h)].astype(F32)
                xg = g_ref[rs, heads(h)].astype(F32)
                for m in range(LB):
                    if i >> m & 1:
                        c = (h * K + L + m) * D
                        w = column(h, rs, span_bits + 1 + m)
                        wq_ref[rs, c : c + D] = (xq * w).astype(BF16)
                        wg_ref[rs, c : c + D] = (xg * w).astype(BF16)
        pulls = [None] * blocks
        for m in range(LB):
            step = 1 << m
            c = (h * K + L + m) * D
            for low in range(0, blocks, 2 * step):
                rs = slice((low + step) * span, (low + 2 * step) * span)
                grad = mm(gt_scr[h, :, rs], wq_ref[rs, c : c + D], NN)
                for i in range(low, low + step):
                    pulls[i] = grad if pulls[i] is None else pulls[i] + grad
        for i in range(blocks):
            pl_scr[i, h] = jnp.zeros((D, D), F32) if pulls[i] is None else pulls[i]

    def unit(h, i):
        hs = heads(h)
        ts = slice(i * span, (i + 1) * span)
        q, k, v, g = q_ref[ts, hs], k_ref[ts, hs], v_ref[ts, hs], g_ref[ts, hs]
        scores = mm(q, k, NT)
        grad_scores = mm(g, v, NT)
        for start in range(0, span, 64):
            rs = slice(start, start + 64)
            wts = slice(i * span + start, i * span + start + 64)
            mask = jnp.zeros((64, span), F32)
            here = lev_scr[rs, :]
            for level in range(span_bits + 1):
                mask = jnp.where(here == level, column(h, wts, level), mask)
            p_scr[rs, :] = (scores[rs, :] * mask).astype(BF16)
            d_scr[rs, :] = (grad_scores[rs, :] * mask).astype(BF16)
        lo_ref[ts, hs] = mm(p_scr[...], v, NN)
        lq_ref[ts, hs] = mm(d_scr[...], k, NN)
        lk_ref[ts, hs] = mm(d_scr[...], q, TN)
        lv_ref[ts, hs] = mm(p_scr[...], g, TN)

    work = [(h, i) for i in range(blocks) for h in range(H)]

    def units(start, end):
        for h, i in work[len(work) * start // 8 : len(work) * end // 8]:
            unit(h, i)

    units(0, CUTS[0])
    pair.wait()
    for j in range(pooled - 1, 0, -1):
        tots[j - 1] = st[j, core] + pin[j - 1]
        if kinds[j] == FLAT:
            start_flat(j, tots.at[j - 1])
        else:
            start_reduce(j, tots.at[j - 1])
    spreads = [j for j in range(top, 0, -1) if kinds[j] != FLAT]
    units(CUTS[0], CUTS[1])
    spread(spreads[0])
    units(CUTS[1], CUTS[2])
    for j in spreads[1:]:
        spread(j)
    units(CUTS[2], CUTS[3])
    def relay(low, high, n):
        ref = far.at[pl.ds(low, high - low), core]
        copy = remote(ref, ref, c_send.at[n], c_recv.at[n], partner)
        copy.start()
        return copy

    flats = [j for j in range(1, L) if kinds[j] == FLAT]
    near.wait()
    for j in flats:
        arrived(j)
    early = relay(1, 1 + len(flats), 0)
    for h in range(H):
        weigh(g_ref, wg_ref, h, range(L))
    units(CUTS[3], 8)
    for h in range(H):
        local_states(h)
    for j in range(1 + len(flats), L):
        arrived(j)
    late = relay(1 + len(flats), L, 1)
    early.wait()

    def gather(h, js, pulled):
        for j in js:
            value = far[j, h]
            up = upper[j] == 1
            pulled = pulled + jnp.where(up, 0.0, value)
            chosen = jnp.where(up, value, 0.0).astype(BF16)
            bnt_ref[h, :, j * D : (j + 1) * D] = chosen
            bnn_ref[h, j * D : (j + 1) * D, :] = chosen
        return pulled

    split = 1 + len(flats)
    for h in range(H):
        s_scr[h] = gather(h, range(split), jnp.zeros((D, D), F32))
    for j in range(1, L):
        settle(j)
    late.wait()
    for h in range(H):
        pulled = gather(h, range(split, L), s_scr[h])
        for i in range(blocks):
            pul_ref[i, h] = (pulled + pl_scr[i, h]).astype(BF16)


def finish_kernel(
    dims, lo, lq, lk, lv, wq, wg, k, v, bnt, bnn, pul, bl,
    out_hbm, dq_hbm, dk_hbm, dv_hbm, out, dq, dk, dv, sem,
):
    H, D, L, span = dims
    blocks = lo.shape[0] // span
    LB = blocks.bit_length() - 1
    K = L + LB
    copies = []
    for i in range(blocks):
        ts = slice(i * span, (i + 1) * span)
        for h in range(H):
            hs = slice(h * D, (h + 1) * D)
            dk[ts, hs] = lk[ts, hs] + mm(v[ts, hs], pul[i, h], NN)
            dv[ts, hs] = lv[ts, hs] + mm(k[ts, hs], pul[i, h], NT)
            ls = slice(h * K * D, (h * K + L) * D)
            o = lo[ts, hs] + mm(wq[ts, ls], bnt[h], NT)
            b = lq[ts, hs] + mm(wg[ts, ls], bnn[h], NN)
            at = 0
            for m in range(LB):
                if i >> m & 1:
                    c = (h * K + L + m) * D
                    state = bl[h, at + (i >> m + 1)]
                    o = o + mm(wq[ts, c : c + D], state, NT)
                    b = b + mm(wg[ts, c : c + D], state, NN)
                at += blocks >> m + 1
            out[ts, hs] = o
            dq[ts, hs] = b
        for n, (src, dst) in enumerate(
            [(dk, dk_hbm), (dv, dv_hbm), (out, out_hbm), (dq, dq_hbm)]
        ):
            copy = pltpu.make_async_copy(src.at[ts], dst.at[ts], sem.at[i, n])
            copy.start()
            copies.append(copy)
    for copy in copies:
        copy.wait()


def shards(cols, rows, queries, keys, values, out_grad, weight_table, profile):
    T = queries.shape[0]
    H = weight_table.shape[1]
    D = queries.shape[1] // H
    levels = weight_table.shape[2]
    L = rows.bit_length() + cols.bit_length() - 2
    profiles = weight_table.shape[0]
    top = L - 1
    kinds = level_kinds(L, D)
    pooled = min([j for j in range(1, L) if kinds[j] == DIRECT], default=L)
    span = min(T, SPAN)
    blocks = T // span
    LB = blocks.bit_length() - 1
    assert H == 2 and L > 2 and H * WIDE == 128 and levels <= WIDE
    pieces = [(8, D)]
    for j in range(1, L):
        n = 1 << j - 1
        R = D if kinds[j] == FLAT else D // min(n, D // 8)
        pieces.append((n * (2 if kinds[j] == DIRECT else 1), R, D))
    vm = pl.BlockSpec(memory_space=pltpu.VMEM)
    sds = jax.ShapeDtypeStruct
    dma = pltpu.SemaphoreType.DMA
    local = sds((T, H * D), F32)
    weighted = sds((T, H * (L + LB) * D), BF16)
    parts = pl.pallas_call(
        functools.partial(main_kernel, (T, H, D, cols, rows, span)),
        out_shape=[
            local, local, local, local, weighted, weighted,
            sds((H, D, L * D), BF16), sds((H, L * D, D), BF16), sds((blocks, H, D, D), BF16),
            sds((H, max(blocks - 1, 1), D, D), BF16),
            sds((T, H * D), BF16), sds((T, H * D), BF16),
        ],
        in_specs=[pl.BlockSpec(memory_space=pltpu.HBM)] * 6,
        out_specs=[vm] * 12,
        scratch_shapes=[
            pltpu.VMEM((T, H * D), BF16),
            pltpu.VMEM((T, H * D), BF16),
            pltpu.VMEM((levels, H, profiles), F32),
            pltpu.VMEM((1, T), jnp.int32),
            dma((6,)),
            pltpu.VMEM((profiles, H * WIDE), F32),
            pltpu.VMEM((T, H * WIDE), F32),
            pltpu.VMEM((span, span), jnp.int32),
            pltpu.VMEM((H, D, T), BF16),
            pltpu.VMEM((span, span), BF16),
            pltpu.VMEM((span, span), BF16),
            pltpu.VMEM((H, D, D), F32),
            pltpu.VMEM((blocks, H, D, D), F32),
            pltpu.VMEM((L, H, D, D), F32),
            pltpu.VMEM((H, D, D), F32),
            pltpu.VMEM((pooled - 1, D, D), F32),
            pltpu.VMEM((pooled - 1, D, D), F32),
            pltpu.VMEM((L, H, D, D), F32),
            [pltpu.VMEM(shape, F32) for shape in pieces],
            [pltpu.VMEM(shape[-2:], F32) for shape in pieces],
            dma((2,)), dma((2,)),
            dma((L,)), dma((L,)),
            dma((L,)), dma((L,)),
            dma((2,)), dma((2,)),
        ],
        compiler_params=pltpu.CompilerParams(
            collective_id=0, has_side_effects=True, vmem_limit_bytes=40 * 1024 * 1024
        ),
        name="main",
    )(*[pltpu.with_memory_space_constraint(a, pltpu.HBM) for a in (queries, keys, values, out_grad, jnp.transpose(weight_table, (2, 1, 0)), profile.reshape(1, T))])
    lo, lq, lk, lv, wq, wg, bnt, bnn, pul, bl, k_near, v_near = parts
    return pl.pallas_call(
        functools.partial(finish_kernel, (H, D, L, span)),
        out_shape=[local] * 4,
        in_specs=[vm] * 12,
        out_specs=[pl.BlockSpec(memory_space=pltpu.HBM)] * 4,
        scratch_shapes=[pltpu.VMEM((T, H * D), F32)] * 4 + [dma((blocks, 4))],
        compiler_params=pltpu.CompilerParams(vmem_limit_bytes=24 * 1024 * 1024),
        name="finish",
    )(lo, lq, lk, lv, wq, wg, k_near, v_near, bnt, bnn, pul, bl)


def solution(mesh):
    tokens = P(("col", "row"), None)
    return jax.shard_map(
        functools.partial(shards, mesh.shape["col"], mesh.shape["row"]),
        mesh=mesh,
        in_specs=(tokens,) * 4 + (P(), P(("col", "row"))),
        out_specs=(tokens,) * 4,
        check_vma=False,
    )
```
